8 devices in a mesh: dp: 2 (over y, z), sp: 4 (over x, core).
Axes of the slice: x: 2, y: 2, z: 1, core: 2. Of those that a mesh axis runs over, the one named last changes fastest.
Arguments:
- x: bfloat16 [8192, 2560], P(('dp', 'sp')), parts along dimension 0
- gain: bfloat16 [2560], replicated
- wq: bfloat16 [2560, 4096], P('sp')
- wk: bfloat16 [2560, 1024], P('sp')
- wv: bfloat16 [2560, 1024], P('sp')
- wo: bfloat16 [4096, 2560], P('sp')
Outputs:
- output: bfloat16 [8192, 2560], P(('dp', 'sp')), parts along dimension 0
There are 2 independent parts. The reference program is written for one: setup_inputs(seed, part) draws one part's arguments, and reference() takes and returns one part's arrays. A program takes and returns all parts, laid end to end along the dimension named above; an argument that names none is the same for every part.
All inputs are finite; a program needn't handle non-finite values.
Results may differ from the reference program's by a relative error of at most 0.012.
Values are sent between devices in bfloat16 or wider.
A program may use at most 2 GiB of HBM per device.

```python
import jax
import jax.numpy as jnp
from jax import lax

ROWS = 4096
D = 2560
HEADS = 32
KV_HEADS = 8
HEAD = 128
THETA = 10000


def setup_inputs(seed: int = 0, part: int = 0) -> dict:
    kx, kn, kq, kk, kv, ko = jax.random.split(jax.random.key(seed), 6)

    def weights(key, rows, columns):
        return jax.random.normal(key, (rows, columns), jnp.float32) * rows**-0.5

    drawn = {
        "x": jax.random.normal(jax.random.fold_in(kx, part), (ROWS, D), jnp.float32),
        "gain": 1 + 0.1 * jax.random.normal(kn, (D,), jnp.float32),
        "wq": 2 * weights(kq, D, HEADS * HEAD),
        "wk": 2 * weights(kk, D, KV_HEADS * HEAD),
        "wv": 4 * weights(kv, D, KV_HEADS * HEAD),
        "wo": weights(ko, HEADS * HEAD, D),
    }
    return {k: v.astype(jnp.bfloat16) for k, v in drawn.items()}


def normed(x, gain):
    wide = x.astype(jnp.float32)
    scale = lax.rsqrt(jnp.mean(wide * wide, -1, keepdims=True) + 1e-6)
    return (wide * scale * gain.astype(jnp.float32)).astype(jnp.bfloat16)


def turned(t, place, theta):
    half = t.shape[-1] // 2
    angle = place.astype(jnp.float32)[:, None] * theta ** (-jnp.arange(half, dtype=jnp.float32) / half)
    cos, sin = jnp.cos(angle)[:, None], jnp.sin(angle)[:, None]
    a, b = t[..., :half].astype(jnp.float32), t[..., half:].astype(jnp.float32)
    return jnp.concatenate([a * cos - b * sin, b * cos + a * sin], -1).astype(jnp.bfloat16)


def matmul(a, w):
    return jnp.dot(a, w, preferred_element_type=jnp.float32).astype(jnp.bfloat16)


def einsum(form, a, b):
    return jnp.einsum(form, a.astype(jnp.float32), b.astype(jnp.float32))


def attention(q, k, v):
    scores = einsum("tgsd,ugd->gstu", q, k) * q.shape[-1] ** -0.5
    token = jnp.arange(q.shape[0])
    scores = jnp.where(token[:, None] >= token, scores, -jnp.inf)
    weights = jax.nn.softmax(scores, -1).astype(jnp.bfloat16)
    return einsum("gstu,ugd->tgsd", weights, v).astype(jnp.bfloat16)


def reference(x, gain, wq, wk, wv, wo):
    a, place = normed(x, gain), jnp.arange(ROWS)
    q = turned(matmul(a, wq).reshape(ROWS, HEADS, HEAD), place, THETA).reshape(ROWS, KV_HEADS, -1, HEAD)
    k = turned(matmul(a, wk).reshape(ROWS, KV_HEADS, HEAD), place, THETA)
    v = matmul(a, wv).reshape(ROWS, KV_HEADS, HEAD)
    seen = attention(q, k, v).reshape(ROWS, HEADS * HEAD)
    return (x.astype(jnp.float32) + jnp.dot(seen, wo, preferred_element_type=jnp.float32)).astype(jnp.bfloat16)
```

```python
import functools

import jax
import jax.numpy as jnp
from jax import lax
from jax.experimental import pallas as pl
from jax.experimental.pallas import tpu as pltpu
from jax.sharding import PartitionSpec as P

NEG = -1e30
HIDDEN = 2 * NEG
LOG2E = 1.4426950408889634
VMEM = 56 * 2**20
STRIP = 512
HEAD = 128
GROUP = 4
THETA = 10000
D = 2560
F32, BF16 = jnp.float32, jnp.bfloat16


def _dot(a, b, ca, cb):
    return lax.dot_general(a, b, (((ca,), (cb,)), ((), ())), preferred_element_type=F32)


def _attend(pos_ref, q_ref, k_ref, v_ref, *rest, causal, scale, bq, bk, carried):
    o_in, lse_in = rest[:2] if carried else (None, None)
    if carried:
        o_ref, top_s, mix_s = rest[-3:]
        lse_ref = gap_s = None
    else:
        o_ref, lse_ref, top_s, mix_s, gap_s = rest[-5:]
    kb, g, d = q_ref.shape[0], q_ref.shape[1], q_ref.shape[3]
    low = k_ref.dtype
    cols = g * bq
    iq = pl.program_id(0)
    e = scale * LOG2E
    wide = min(cols, STRIP)
    pieces = [(i, at) for i in range(kb) for at in range(0, cols, wide)]

    if causal:
        gap_s[...] = lax.rem(lax.broadcasted_iota(jnp.int32, (bk, cols), 1), bq) - lax.broadcasted_iota(jnp.int32, (bk, cols), 0)
    for i in range(kb):
        if carried:
            for n in range(g):
                h = i * g + n
                top_s[i : i + 1, n * bq : (n + 1) * bq] = jnp.maximum(lse_in[h : h + 1, :] * (1 / scale), NEG)
                mix_s[i, :d, n * bq : (n + 1) * bq] = o_in[:, h * d : (h + 1) * d].T
            mix_s[i, d:, :] = jnp.ones((8, cols), F32)
        else:
            top_s[i : i + 1, :] = jnp.full((1, cols), NEG, F32)
            mix_s[i] = jnp.zeros((d + 8, cols), F32)
    ones = jnp.ones((8, bk), low)

    def block(j, masked):
        here = pl.ds(j * bk, bk)
        scores = [_dot(k_ref[i, here, :], q_ref[i].reshape(cols, d)[at : at + wide, :], 1, 1) for i, at in pieces]
        ok = gap_s[...] >= j * bk - iq * bq if masked else None
        weights, keeps = [], []
        for (i, at), s in zip(pieces, scores):
            if masked:
                s = jnp.where(ok[:, at : at + wide], s, HIDDEN)
            old = top_s[i : i + 1, at : at + wide]
            top = jnp.maximum(old, s.max(axis=0, keepdims=True))
            top_s[i : i + 1, at : at + wide] = top
            weights.append(jnp.exp2((s - top) * e).astype(low))
            keeps.append(jnp.exp2((old - top) * e))
        for (i, at), p, keep in zip(pieces, weights, keeps):
            values = jnp.concatenate([v_ref[i, here, :].T, ones], axis=0)
            mix_s[i, :, at : at + wide] = mix_s[i, :, at : at + wide] * keep + _dot(values, p, 1, 0)

    if causal:
        whole, last = lax.div(iq * bq + 1, bk), lax.div(iq * bq + bq - 1 + bk, bk)
        lax.fori_loop(0, whole, lambda j, _: block(j, False), None)
        lax.fori_loop(whole, last, lambda j, _: block(j, True), None)
    else:
        lax.fori_loop(0, lax.div(pos_ref[0], bk), lambda j, _: block(j, False), None)

    for i in range(kb):
        top, total = top_s[i : i + 1, :], mix_s[i, d : d + 1, :]
        out = mix_s[i, :d, :] * (1 / total)
        if not carried:
            lse = top * scale + jnp.log(total)
        for n in range(g):
            h, part = i * g + n, slice(n * bq, (n + 1) * bq)
            o_ref[:, h * d : (h + 1) * d] = out[:, part].T.astype(o_ref.dtype)
            if not carried:
                lse_ref[h : h + 1, :] = lse[:, part]


def attend(q, kv, *, causal, keys=None, carry=None, bq=512, bk=512):
    kb, g, sq, d = q.shape
    sk = kv.shape[1]
    h = kb * g
    carried = carry is not None
    whole = lambda at: pl.BlockSpec((kb, sk, d), lambda iq, _: (at, 0, 0))
    rows = pl.BlockSpec((bq, h * d), lambda iq, _: (iq, 0))
    stats = pl.BlockSpec((h, bq), lambda iq, _: (0, iq))
    specs = [pl.BlockSpec((kb, g, bq, d), lambda iq, _: (0, 0, iq, 0)), whole(0), whole(1)] + ([rows, stats] if carried else [])
    out_shape = [jax.ShapeDtypeStruct((sq, h * d), BF16 if carried else F32)]
    out_specs = [rows]
    scratch = [pltpu.VMEM((kb, g * bq), F32), pltpu.VMEM((kb, d + 8, g * bq), F32)]
    if not carried:
        out_shape.append(jax.ShapeDtypeStruct((h, sq), F32))
        out_specs.append(stats)
        scratch.append(pltpu.VMEM((bk, g * bq), jnp.int32))
    keys = jnp.full((1,), sk if keys is None else keys, jnp.int32)
    out = pl.pallas_call(
        functools.partial(_attend, causal=causal, scale=d**-0.5, bq=bq, bk=bk, carried=carried),
        grid_spec=pltpu.PrefetchScalarGridSpec(num_scalar_prefetch=1, grid=(sq // bq,), in_specs=specs, out_specs=out_specs, scratch_shapes=scratch),
        out_shape=out_shape,
        compiler_params=pltpu.CompilerParams(dimension_semantics=("arbitrary",), vmem_limit_bytes=VMEM),
        cost_estimate=pl.CostEstimate(flops=4 * h * sq * sk * d // (2 if causal else 1), transcendentals=h * sq * sk, bytes_accessed=16 * 2**20),
        name="attend_far" if carried else "attend_near",
    )(keys, q, kv, kv, *(carry or ()))
    return out[0] if carried else out


def normed(x, gain):
    wide = x.astype(F32)
    scale = lax.rsqrt(jnp.mean(wide * wide, -1, keepdims=True) + 1e-6)
    return (wide * scale * gain.astype(F32)).astype(BF16)


def _place():
    g, sp = lax.axis_index("dp"), lax.axis_index("sp")
    return g, sp // 2, sp % 2


def _project(a_ref, cos_ref, sin_ref, *rest, plan, turn):
    pieces, (out_ref, w_s, sems) = rest[:-3], rest[-3:]

    @pl.when(pl.program_id(0) == 0)
    def _():
        copies = []
        for n, (ref, col, width, row, to) in enumerate(plan(*_place())):
            src = pieces[ref].at[:, pl.ds(pl.multiple_of(col, 128), width)]
            dst = w_s.at[pl.ds(pl.multiple_of(row, 128), src.shape[0]), pl.ds(pl.multiple_of(to, 128), width)]
            copies.append(pltpu.make_async_copy(src, dst, sems.at[n]))
        for copy in copies:
            copy.start()
        for copy in copies:
            copy.wait()

    acc = jnp.dot(a_ref[...], w_s[...], preferred_element_type=F32).astype(BF16)
    cos, sin = cos_ref[...], sin_ref[...]
    for h in range(out_ref.shape[0]):
        t = acc[:, h * HEAD : (h + 1) * HEAD]
        if turn(h):
            t = t.astype(F32)
            t = (t * cos + pltpu.roll(t, HEAD // 2, 1) * sin).astype(BF16)
        out_ref[h] = t


def project(a, cos, sin, pieces, plan, copies, heads, turn, name, bt=256):
    tokens = a.shape[0]
    width = heads * HEAD
    return pl.pallas_call(
        functools.partial(_project, plan=plan, turn=turn),
        grid=(tokens // bt,),
        in_specs=[pl.BlockSpec((bt, D), lambda i: (i, 0))] + [pl.BlockSpec((bt, HEAD), lambda i: (i, 0))] * 2
        + [pl.BlockSpec(memory_space=pl.ANY)] * len(pieces),
        out_specs=pl.BlockSpec((heads, bt, HEAD), lambda i: (0, i, 0)),
        out_shape=jax.ShapeDtypeStruct((heads, tokens, HEAD), BF16),
        scratch_shapes=[pltpu.VMEM((D, width), BF16), pltpu.SemaphoreType.DMA((copies,))],
        compiler_params=pltpu.CompilerParams(dimension_semantics=("arbitrary",), vmem_limit_bytes=VMEM),
        cost_estimate=pl.CostEstimate(flops=2 * tokens * D * width, transcendentals=0, bytes_accessed=2 * (tokens * D + D * width + tokens * width)),
        name=name,
    )(a, cos, sin, *pieces)


def _finish(tok_ref, s0_ref, s1_ref, *rest, half, last):
    if last:
        x_ref, got_ref = rest[:2]
        rest = rest[2:]
        own, wx, wy = rest[:3]
    else:
        own, wx, wy = rest[:3]
    out_ref, w_s, sems = rest[-3:]
    width = w_s.shape[1]

    @pl.when(pl.program_id(0) == 0)
    def _():
        g, s, _ = _place()
        first = pltpu.make_async_copy(own.at[:, pl.ds(half * width, width)], w_s.at[pl.ds(pl.multiple_of(s * 1024, 1024), 1024)], sems.at[0])
        there = w_s.at[pl.ds(pl.multiple_of((1 - s) * 1024, 1024), 1024)]
        first.start()

        @pl.when(g == half)
        def _():
            c = pltpu.make_async_copy(wx, there, sems.at[1])
            c.start()
            c.wait()

        @pl.when(g != half)
        def _():
            c = pltpu.make_async_copy(wy, there, sems.at[1])
            c.start()
            c.wait()

        first.wait()

    seen = jnp.concatenate([s0_ref[...], s1_ref[...]], axis=1)
    acc = jnp.dot(seen, w_s[...], preferred_element_type=F32)
    if last:
        out_ref[...] = (x_ref[...].astype(F32) + (acc + got_ref[...])).astype(BF16)
    else:
        out_ref[...] = acc


def finish(seen, wo, wx, wy, start, half, x=None, got=None, into=None, bt=256):
    rows, width = 1024, D // 2
    last = x is not None
    tok = jnp.full((1,), start, jnp.int32)
    some = pl.BlockSpec((bt, 1024), lambda i, tok: (tok[0] + i, 0))
    here = pl.BlockSpec((bt, width), lambda i, tok: (i, half))
    anywhere = pl.BlockSpec(memory_space=pl.ANY)
    args = [*seen] + ([x, got] if last else []) + [wo, wx, wy] + ([into] if into is not None else [])
    specs = [some, some] + ([here, pl.BlockSpec((bt, width), lambda i, tok: (i, 0))] if last else []) + [anywhere] * (3 + (into is not None))
    return pl.pallas_call(
        functools.partial(_finish, half=half, last=last),
        grid_spec=pltpu.PrefetchScalarGridSpec(
            num_scalar_prefetch=1, grid=(rows // bt,), in_specs=specs,
            out_specs=here if last else pl.BlockSpec((bt, width), lambda i, tok: (i, 0)),
            scratch_shapes=[pltpu.VMEM((2048, width), BF16), pltpu.SemaphoreType.DMA((2,))]),
        out_shape=jax.ShapeDtypeStruct((rows, D), BF16) if last else jax.ShapeDtypeStruct((rows, width), F32),
        input_output_aliases={len(args): 0} if into is not None else {},
        compiler_params=pltpu.CompilerParams(dimension_semantics=("arbitrary",), vmem_limit_bytes=VMEM),
        cost_estimate=pl.CostEstimate(flops=2 * rows * 2048 * width, transcendentals=0, bytes_accessed=20 * 2**20),
        name=f"finish_{'own' if last else 'other'}{half}",
    )(tok, *args)


def _pairs(to):
    spots = [(g, s, c) for g in range(2) for s in range(2) for c in range(2)]
    flat = lambda t: 4 * t[0] + 2 * t[1] + t[2]
    return [(flat(t), flat(to(*t))) for t in spots if to(*t) is not None]


SAME = _pairs(lambda g, s, c: (g, 1 - s, c))
CROSS = _pairs(lambda g, s, c: (g, 1 - s, 1 - c))
MATE = _pairs(lambda g, s, c: (g, s, 1 - c))
TWIN = _pairs(lambda g, s, c: (1 - g, s, c))
AHEAD = _pairs(lambda g, s, c: (g, 1, c) if s == 0 else None)


def send(t, pairs):
    return lax.ppermute(t, ("dp", "sp"), pairs)


def columns(w, at, size):
    return lax.dynamic_slice_in_dim(w, at, size, axis=1)


SPLIT = 2


def step(x, gain, wq, wk, wv, wo):
    g, s, c = _place()
    own = x.shape[0]

    def both(at, size):
        return jnp.concatenate([columns(wk, at, size), columns(wv, at, size)], axis=1)

    mate_x = send(x, MATE)
    far_kv, mate_kv, far_q, mate_q = {}, {}, {}, {}
    part = 512 // SPLIT
    for a in range(2):
        mine = [send(both((4 * a + 2 * cc + g) * HEAD, HEAD), p) for cc, p in ((c, SAME), (1 - c, CROSS))]
        far_kv[a] = mine
        mate_kv[a] = send(both((4 * a + 2 * (1 - c)) * HEAD, 2 * HEAD), MATE)
        far_q[a] = [[send(columns(wq, (4 * a + 2 * cc + g) * 512 + n * part, part), p) for cc, p in ((c, SAME), (1 - c, CROSS))]
                    for n in range(SPLIT)]
        mate_q[a] = send(columns(wq, (4 * a + 2 * (1 - c)) * 512, 1024), MATE)
    for a in range(2):
        far_kv[a] = far_kv[a] + [send(t, TWIN) for t in far_kv[a]]
        far_q[a] = [t + [send(u, TWIN) for u in t] for t in far_q[a]]

    tokens = 2 * own
    low, high = jnp.where(c == 0, x, mate_x), jnp.where(c == 0, mate_x, x)
    act = normed(jnp.concatenate([low, high]), gain)
    place = (s * tokens + jnp.arange(tokens)).astype(F32)
    angle = place[:, None] * THETA ** (-jnp.arange(HEAD // 2, dtype=F32) / (HEAD // 2))
    cos, sin = jnp.cos(angle), jnp.sin(angle)
    cos, sin = jnp.concatenate([cos, cos], 1), jnp.concatenate([-sin, sin], 1)

    def row(s, c):
        return (2 * s + c) * 640

    def kv_plan(a):
        def plan(g, s, c):
            at = (4 * a + 2 * c) * HEAD
            out = [(0, at, 256, row(s, c), 0), (1, at, 256, row(s, c), 256), (2, 0, 512, row(s, 1 - c), 0)]
            for ref, (r, cc) in enumerate(((g, c), (g, 1 - c), (1 - g, c), (1 - g, 1 - c)), 3):
                out += [(ref, 0, HEAD, row(1 - s, cc), r * HEAD), (ref, HEAD, HEAD, row(1 - s, cc), 256 + r * HEAD)]
            return out
        return plan

    def q_plan(a):
        def plan(g, s, c):
            out = [(0, (4 * a + 2 * c) * 512, 1024, row(s, c), 0), (1, 0, 1024, row(s, 1 - c), 0)]
            for n in range(SPLIT):
                for ref, (r, cc) in enumerate(((g, c), (g, 1 - c), (1 - g, c), (1 - g, 1 - c)), 2 + 4 * n):
                    out.append((ref, 0, part, row(1 - s, cc), r * 512 + n * part))
            return out
        return plan

    def keys_values(a):
        return project(act, cos, sin, [wk, wv, mate_kv[a], *far_kv[a]], kv_plan(a), 11, 4, lambda h: h < 2, "kv_proj")

    def queries(a):
        got = project(act, cos, sin, [wq, mate_q[a], *sum(far_q[a], [])], q_plan(a), 2 + 4 * SPLIT, 8, lambda h: True, "q_proj")
        return got.reshape(2, GROUP, tokens, HEAD)

    kv, q, near, there = {}, {}, {}, {}
    for a in range(2):
        kv[a] = keys_values(a)
        there[a] = send(kv[a], AHEAD)
        q[a] = queries(a)
        near[a] = attend(q[a], kv[a], causal=True)
    wo_out, _ = lax.optimization_barrier((wo, kv[1]))
    wx = send(columns(wo_out, g * (D // 2), D // 2), SAME)
    wy = send(wx, TWIN)
    seen = [attend(q[a], there[a], causal=False, keys=s * tokens, carry=near[a], bk=1024) for a in range(2)]

    blocks = own // 256
    got = [send(finish(seen, wo, wx, wy, (1 - c) * blocks, half), MATE) for half in range(2)]
    y = finish(seen, wo, wx, wy, c * blocks, 0, x, got[0])
    return finish(seen, wo, wx, wy, c * blocks, 1, x, got[1], into=y)


def solution(mesh):
    tokens, whole = P(("dp", "sp"), None), P("sp", None)
    return jax.shard_map(step, mesh=mesh, in_specs=(tokens, P(None), whole, whole, whole, whole), out_specs=tokens, check_vma=False)
```

```python
import functools

import jax
import jax.numpy as jnp
from jax import lax
from jax.experimental import pallas as pl
from jax.experimental.pallas import tpu as pltpu
from jax.sharding import PartitionSpec as P


NEG = -1e30
HIDDEN = 2 * NEG
LOG2E = 1.4426950408889634
VMEM = 56 * 2**20
STRIP = 512
HEAD = 128
GROUP = 4
THETA = 10000
BT = 512
D = 2560
F32, BF16 = jnp.float32, jnp.bfloat16


def _dot(a, b, ca, cb):
    return lax.dot_general(a, b, (((ca,), (cb,)), ((), ())), preferred_element_type=F32)


def _attend(pos_ref, q_ref, k_ref, v_ref, *rest, causal, scale, bq, bk, carried):
    o_in, lse_in = rest[:2] if carried else (None, None)
    if carried:
        o_ref, top_s, mix_s = rest[-3:]
        lse_ref = gap_s = None
    else:
        o_ref, lse_ref, top_s, mix_s, gap_s = rest[-5:]
    kb, g, d = q_ref.shape[0], q_ref.shape[1], q_ref.shape[3]
    low = k_ref.dtype
    cols = g * bq
    iq = pl.program_id(0)
    e = scale * LOG2E
    wide = min(cols, STRIP)
    pieces = [(i, at) for i in range(kb) for at in range(0, cols, wide)]

    if causal:
        gap_s[...] = lax.rem(lax.broadcasted_iota(jnp.int32, (bk, cols), 1), bq) - lax.broadcasted_iota(jnp.int32, (bk, cols), 0)
    for i in range(kb):
        if carried:
            for n in range(g):
                h = i * g + n
                top_s[i : i + 1, n * bq : (n + 1) * bq] = jnp.maximum(lse_in[h : h + 1, :] * (1 / scale), NEG)
                mix_s[i, :d, n * bq : (n + 1) * bq] = o_in[:, h * d : (h + 1) * d].T
            mix_s[i, d:, :] = jnp.ones((8, cols), F32)
        else:
            top_s[i : i + 1, :] = jnp.full((1, cols), NEG, F32)
            mix_s[i] = jnp.zeros((d + 8, cols), F32)
    ones = jnp.ones((8, bk), low)

    def block(j, masked):
        here = pl.ds(j * bk, bk)
        scores = [_dot(k_ref[i, here, :], q_ref[i].reshape(cols, d)[at : at + wide, :], 1, 1) for i, at in pieces]
        ok = gap_s[...] >= j * bk - iq * bq if masked else None
        weights, keeps = [], []
        for (i, at), s in zip(pieces, scores):
            if masked:
                s = jnp.where(ok[:, at : at + wide], s, HIDDEN)
            old = top_s[i : i + 1, at : at + wide]
            top = jnp.maximum(old, s.max(axis=0, keepdims=True))
            top_s[i : i + 1, at : at + wide] = top
            weights.append(jnp.exp2((s - top) * e).astype(low))
            keeps.append(jnp.exp2((old - top) * e))
        for (i, at), p, keep in zip(pieces, weights, keeps):
            values = jnp.concatenate([v_ref[i, here, :].T, ones], axis=0)
            mix_s[i, :, at : at + wide] = mix_s[i, :, at : at + wide] * keep + _dot(values, p, 1, 0)

    if causal:
        whole, last = lax.div(iq * bq + 1, bk), lax.div(iq * bq + bq - 1 + bk, bk)
        lax.fori_loop(0, whole, lambda j, _: block(j, False), None)
        lax.fori_loop(whole, last, lambda j, _: block(j, True), None)
    else:
        lax.fori_loop(0, lax.div(pos_ref[0], bk), lambda j, _: block(j, False), None)

    for i in range(kb):
        top, total = top_s[i : i + 1, :], mix_s[i, d : d + 1, :]
        out = mix_s[i, :d, :] * (1 / total)
        if not carried:
            lse = top * scale + jnp.log(total)
        for n in range(g):
            h, part = i * g + n, slice(n * bq, (n + 1) * bq)
            o_ref[:, h * d : (h + 1) * d] = out[:, part].T.astype(o_ref.dtype)
            if not carried:
                lse_ref[h : h + 1, :] = lse[:, part]


def attend(q, kv, *, causal, keys=None, carry=None, bq=512, bk=512):
    kb, g, sq, d = q.shape
    sk = kv.shape[1]
    h = kb * g
    carried = carry is not None
    whole = lambda at: pl.BlockSpec((kb, sk, d), lambda iq, _: (at, 0, 0))
    rows = pl.BlockSpec((bq, h * d), lambda iq, _: (iq, 0))
    stats = pl.BlockSpec((h, bq), lambda iq, _: (0, iq))
    specs = [pl.BlockSpec((kb, g, bq, d), lambda iq, _: (0, 0, iq, 0)), whole(0), whole(1)] + ([rows, stats] if carried else [])
    out_shape = [jax.ShapeDtypeStruct((sq, h * d), BF16 if carried else F32)]
    out_specs = [rows]
    scratch = [pltpu.VMEM((kb, g * bq), F32), pltpu.VMEM((kb, d + 8, g * bq), F32)]
    if not carried:
        out_shape.append(jax.ShapeDtypeStruct((h, sq), F32))
        out_specs.append(stats)
        scratch.append(pltpu.VMEM((bk, g * bq), jnp.int32))
    keys = jnp.full((1,), sk if keys is None else keys, jnp.int32)
    out = pl.pallas_call(
        functools.partial(_attend, causal=causal, scale=d**-0.5, bq=bq, bk=bk, carried=carried),
        grid_spec=pltpu.PrefetchScalarGridSpec(num_scalar_prefetch=1, grid=(sq // bq,), in_specs=specs, out_specs=out_specs, scratch_shapes=scratch),
        out_shape=out_shape,
        compiler_params=pltpu.CompilerParams(dimension_semantics=("arbitrary",), vmem_limit_bytes=VMEM),
        cost_estimate=pl.CostEstimate(flops=4 * h * sq * sk * d // (2 if causal else 1), transcendentals=h * sq * sk, bytes_accessed=16 * 2**20),
        name="attend_far" if carried else "attend_near",
    )(keys, q, kv, kv, *(carry or ()))
    return out[0] if carried else out


def _place():
    g, sp = lax.axis_index("dp"), lax.axis_index("sp")
    return g, sp // 2, sp % 2


def _norm(core_ref, x_ref, mate_ref, gain_ref, out_ref):
    def one(ref):
        wide = ref[...].astype(F32)
        scale = lax.rsqrt(jnp.mean(wide * wide, -1, keepdims=True) + 1e-6)
        out_ref[...] = (wide * scale * gain_ref[...].astype(F32)).astype(BF16)

    own = pl.program_id(0) < pl.num_programs(0) // 2

    @pl.when(own)
    def _():
        one(x_ref)

    @pl.when(jnp.logical_not(own))
    def _():
        one(mate_ref)


def norm(x, mate, gain, c, bt=256):
    n = x.shape[0] // bt
    at = lambda j, core: (jnp.where(j < n, core[0] * n + j, (1 - core[0]) * n + j - n), 0)
    return pl.pallas_call(
        _norm,
        grid_spec=pltpu.PrefetchScalarGridSpec(
            num_scalar_prefetch=1, grid=(2 * n,),
            in_specs=[pl.BlockSpec((bt, D), lambda j, core: (jnp.minimum(j, n - 1), 0)), pl.BlockSpec((bt, D), lambda j, core: (jnp.maximum(j - n, 0), 0)),
                      pl.BlockSpec((1, D), lambda j, core: (0, 0))],
            out_specs=pl.BlockSpec((bt, D), at)),
        out_shape=jax.ShapeDtypeStruct((2 * x.shape[0], D), BF16),
        compiler_params=pltpu.CompilerParams(dimension_semantics=("arbitrary",)),
        cost_estimate=pl.CostEstimate(flops=8 * 2 * x.size, transcendentals=0, bytes_accessed=8 * x.size),
        name="norm",
    )(jnp.full((1,), c, jnp.int32), x, mate, gain.reshape(1, D))


def _pack(at_ref, wq_ref, wk_ref, wv_ref, *outs, plans):
    refs = (wq_ref, wk_ref, wv_ref)
    flag = at_ref[at_ref.shape[0] - 1]
    n = 0
    for out, plan in zip(outs, plans):
        to = 0
        for ref, width in plan:
            here = pl.ds(pl.multiple_of(at_ref[n], 128), width)
            if ref < 3:
                out[:, to : to + width] = refs[ref][:, here]
            else:
                out[:, to : to + width] = jnp.where(flag == 0, wk_ref[:, here], wv_ref[:, here])
            to += width
            n += 1


def pack(wq, wk, wv, wanted, half):
    rows, bt = wq.shape[0], 128
    plans = [[(m, w) for m, _, w in want] for want in wanted]
    at = jnp.stack([jnp.asarray(col, jnp.int32) for want in wanted for _, col, _ in want] + [jnp.asarray(half, jnp.int32)])
    widths = [sum(w for _, w in plan) for plan in plans]
    spec = lambda n: pl.BlockSpec((bt, n), lambda i, _: (i, 0))
    return pl.pallas_call(
        functools.partial(_pack, plans=plans),
        grid_spec=pltpu.PrefetchScalarGridSpec(num_scalar_prefetch=1, grid=(rows // bt,), in_specs=[spec(w.shape[1]) for w in (wq, wk, wv)],
                                               out_specs=[spec(n) for n in widths]),
        out_shape=[jax.ShapeDtypeStruct((rows, n), BF16) for n in widths],
        compiler_params=pltpu.CompilerParams(dimension_semantics=("arbitrary",)),
        cost_estimate=pl.CostEstimate(flops=rows * sum(widths), transcendentals=0, bytes_accessed=8 * rows * sum(widths)),
    )(at, wq, wk, wv)


def _project(a_ref, cos_ref, sin_ref, *rest, plan):
    pieces, (q_ref, kv_ref, w_s, sems) = rest[:-4], rest[-4:]

    @pl.when(pl.program_id(0) == 0)
    def _():
        copies = []
        for n, (ref, col, width, row, to) in enumerate(plan):
            src = pieces[ref].at[:, pl.ds(col if isinstance(col, int) else pl.multiple_of(col, 128), width)]
            dst = w_s.at[pl.ds(pl.multiple_of(row, 128), src.shape[0]), pl.ds(to if isinstance(to, int) else pl.multiple_of(to, 128), width)]
            copies.append(pltpu.make_async_copy(src, dst, sems.at[n]))
        for copy in copies:
            copy.start()
        for copy in copies:
            copy.wait()

    cos, sin = cos_ref[...], sin_ref[...]
    acc = jnp.dot(a_ref[...], w_s[...], preferred_element_type=F32).astype(BF16)
    nq, nk = q_ref.shape[0], kv_ref.shape[0] // 2
    for h in range(nq + 2 * nk):
        t = acc[:, h * HEAD : (h + 1) * HEAD]
        if h < nq + nk:
            t = t.astype(F32)
            t = (t * cos + pltpu.roll(t, HEAD // 2, 1) * sin).astype(BF16)
        if h < nq:
            q_ref[h] = t
        else:
            kv_ref[h - nq] = t


def project(a, cos, sin, pieces, plan, kb, bt=256):
    tokens = a.shape[0]
    nq, nkv = kb * GROUP, 2 * kb
    width = (nq + nkv) * HEAD
    count = len(plan(0, 0, 0))
    return pl.pallas_call(
        lambda *refs: _project(*refs, plan=plan(*_place())),
        grid=(tokens // bt,),
        in_specs=[pl.BlockSpec((bt, D), lambda i: (i, 0))] + [pl.BlockSpec((bt, HEAD), lambda i: (i, 0))] * 2
        + [pl.BlockSpec(memory_space=pl.ANY)] * len(pieces),
        out_specs=[pl.BlockSpec((nq, bt, HEAD), lambda i: (0, i, 0)), pl.BlockSpec((nkv, bt, HEAD), lambda i: (0, i, 0))],
        out_shape=[jax.ShapeDtypeStruct((nq, tokens, HEAD), BF16), jax.ShapeDtypeStruct((nkv, tokens, HEAD), BF16)],
        scratch_shapes=[pltpu.VMEM((D, width), BF16), pltpu.SemaphoreType.DMA((count,))],
        compiler_params=pltpu.CompilerParams(dimension_semantics=("arbitrary",), vmem_limit_bytes=VMEM),
        cost_estimate=pl.CostEstimate(flops=2 * tokens * D * width, transcendentals=0, bytes_accessed=2 * (tokens * D + D * width + tokens * width)),
    )(a, cos, sin, *pieces)


def _finish(tok_ref, s0_ref, s1_ref, s2_ref, *rest, half, last):
    if last:
        x_ref, got_ref = rest[:2]
        rest = rest[2:]
    own, far = rest[0], rest[1:5]
    out_ref, w_s, sems = rest[-3:]
    width = w_s.shape[1]

    @pl.when(pl.program_id(0) == 0)
    def _():
        g, s, _ = _place()
        first = pltpu.make_async_copy(own.at[:, pl.ds(half * width, width)], w_s.at[pl.ds(pl.multiple_of(s * 1024, 1024), 1024)], sems.at[0])
        first.start()

        def fetch(parts):
            copies = [pltpu.make_async_copy(t, w_s.at[pl.ds(pl.multiple_of((1 - s) * 1024 + n * 512, 512), 512)], sems.at[1 + n]) for n, t in enumerate(parts)]
            for copy in copies:
                copy.start()
            for copy in copies:
                copy.wait()

        @pl.when(g == half)
        def _():
            fetch(far[:2])

        @pl.when(g != half)
        def _():
            fetch(far[2:])

        first.wait()

    seen = jnp.concatenate([s0_ref[...], s1_ref[...], s2_ref[...]], axis=1)
    acc = jnp.dot(seen, w_s[...], preferred_element_type=F32)
    if last:
        out_ref[...] = (x_ref[...].astype(F32) + (acc + got_ref[...])).astype(BF16)
    else:
        out_ref[...] = acc


def finish(seen, wo, wx, wy, start, half, x=None, got=None, into=None):
    rows, width, bt = 1024, D // 2, BT
    last = x is not None
    tok = jnp.full((1,), start, jnp.int32)
    some = [pl.BlockSpec((bt, t.shape[1]), lambda i, tok: (tok[0] + i, 0)) for t in seen]
    here = pl.BlockSpec((bt, width), lambda i, tok: (i, half))
    anywhere = pl.BlockSpec(memory_space=pl.ANY)
    args = [*seen] + ([x, got] if last else []) + [wo, *wx, *wy] + ([into] if into is not None else [])
    specs = some + ([here, pl.BlockSpec((bt, width), lambda i, tok: (i, 0))] if last else []) + [anywhere] * (5 + (into is not None))
    return pl.pallas_call(
        functools.partial(_finish, half=half, last=last),
        grid_spec=pltpu.PrefetchScalarGridSpec(
            num_scalar_prefetch=1, grid=(rows // bt,), in_specs=specs,
            out_specs=here if last else pl.BlockSpec((bt, width), lambda i, tok: (i, 0)),
            scratch_shapes=[pltpu.VMEM((2048, width), BF16), pltpu.SemaphoreType.DMA((3,))]),
        out_shape=jax.ShapeDtypeStruct((rows, D), BF16) if last else jax.ShapeDtypeStruct((rows, width), F32),
        input_output_aliases={len(args): 0} if into is not None else {},
        compiler_params=pltpu.CompilerParams(dimension_semantics=("arbitrary",), vmem_limit_bytes=VMEM),
        cost_estimate=pl.CostEstimate(flops=2 * rows * 2048 * width, transcendentals=0, bytes_accessed=20 * 2**20),
    )(tok, *args)


def _pairs(to):
    spots = [(g, s, c) for g in range(2) for s in range(2) for c in range(2)]
    flat = lambda t: 4 * t[0] + 2 * t[1] + t[2]
    return [(flat(t), flat(to(*t))) for t in spots if to(*t) is not None]


SAME = _pairs(lambda g, s, c: (g, 1 - s, c))
CROSS = _pairs(lambda g, s, c: (g, 1 - s, 1 - c))
MATE = _pairs(lambda g, s, c: (g, s, 1 - c))
TWIN = _pairs(lambda g, s, c: (1 - g, s, c))
AHEAD = _pairs(lambda g, s, c: (g, 1, c) if s == 0 else None)


def send(t, pairs):
    return lax.ppermute(t, ("dp", "sp"), pairs)


def step(x, gain, wq, wk, wv, wo):
    g, s, c = _place()
    own = x.shape[0]
    tokens = 2 * own
    units = ((0, (0,)), (0, (1,)), (1, (0, 1)))

    def share(unit, cc, half):
        a, rs = unit
        if len(rs) == 1:
            head = 4 * a + 2 * cc + rs[0]
            return [(0, head * 512 + half * 256, 256), (3, head * HEAD, HEAD)]
        head = 4 * a + 2 * cc + half
        return [(0, head * 512, 512), (1, head * HEAD, HEAD), (2, head * HEAD, HEAD)]

    def all_of(unit, cc):
        a, rs = unit
        n = len(rs)
        head = 4 * a + 2 * cc + rs[0]
        return [(0, head * 512, 512 * n), (1, head * HEAD, HEAD * n), (2, head * HEAD, HEAD * n)]

    def row(s, c):
        return (2 * s + c) * 640

    def plan_of(unit):
        n = len(unit[1])
        kv = 512 * n

        def plan(g, s, c):
            out, to = [], 0
            for ref, (_, col, width) in enumerate(all_of(unit, c)):
                out.append((ref, col, width, row(s, c), to))
                to += width
            out.append((3, 0, to, row(s, 1 - c), 0))
            for ref, (half, cc) in enumerate(((g, c), (g, 1 - c), (1 - g, c), (1 - g, 1 - c)), 4):
                if n == 1:
                    parts = [(0, 256, half * 256), (256, HEAD, kv + half * HEAD)]
                else:
                    parts = [(0, 512, half * 512), (512, HEAD, kv + half * HEAD), (512 + HEAD, HEAD, kv + (2 + half) * HEAD)]
                out += [(ref, col, width, row(1 - s, cc), to) for col, width, to in parts]
            return out

        return plan

    mate_x = send(x, MATE)
    far, mate = [], []
    for unit in units:
        got = pack(wq, wk, wv, [share(unit, c, g), share(unit, 1 - c, g), all_of(unit, 1 - c)], g)
        far.append([send(t, pairs) for t, pairs in zip(got, (SAME, CROSS))])
        mate.append(send(got[2], MATE))

    act = norm(x, mate_x, gain, c)
    place = (s * tokens + jnp.arange(tokens)).astype(F32)
    angle = place[:, None] * THETA ** (-jnp.arange(HEAD // 2, dtype=F32) / (HEAD // 2))
    cos, sin = jnp.cos(angle), jnp.sin(angle)
    cos, sin = jnp.concatenate([cos, cos], 1), jnp.concatenate([-sin, sin], 1)

    def relay(n, m, after):
        piece, _ = lax.optimization_barrier((far[n][m], after))
        return send(piece, TWIN)

    def project_unit(n, twin, act):
        q, kv = project(act, cos, sin, [wq, wk, wv, mate[n], *far[n], *twin], plan_of(units[n]), len(units[n][1]))
        return q.reshape(-1, GROUP, tokens, HEAD), kv

    def near_unit(n):
        return attend(q[n], kv[n], causal=True)

    q, kv, near = [None] * 3, [None] * 3, [None] * 3
    twin = [[relay(0, 0, act), relay(0, 1, act)], [relay(1, 0, act)], []]
    q[0], kv[0] = project_unit(0, twin[0], act)
    twin[1].append(relay(1, 1, kv[0]))
    near[0] = near_unit(0)
    twin[2].append(relay(2, 0, near[0][1]))
    q[1], kv[1] = project_unit(1, twin[1], act)
    twin[2].append(relay(2, 1, kv[1]))
    near[1] = near_unit(1)
    q[2], kv[2] = project_unit(2, twin[2], lax.optimization_barrier((act, near[1][1]))[0])
    near[2] = near_unit(2)
    there = [send(t, AHEAD) for t in kv]

    wx, wy = [], []
    for n, after in enumerate((near[0][1], near[1][1])):
        part, _ = lax.optimization_barrier((wo, after))
        part = lax.dynamic_slice(part, (n * 512, g * (D // 2)), (512, D // 2))
        wx.append(send(part, SAME))
    seen = []
    for n in range(3):
        if n < 2:
            part, _ = lax.optimization_barrier((wx[n], near[2][1] if n == 0 else seen[0]))
            wy.append(send(part, TWIN))
        seen.append(attend(q[n], there[n], causal=False, keys=s * tokens, carry=near[n], bk=1024, bq=1024 if n < 2 else 512))

    blocks = own // BT
    got = [send(finish(seen, wo, wx, wy, (1 - c) * blocks, half), MATE) for half in range(2)]
    y = finish(seen, wo, wx, wy, c * blocks, 0, x, got[0])
    return finish(seen, wo, wx, wy, c * blocks, 1, x, got[1], into=y)


def solution(mesh):
    tokens, whole = P(("dp", "sp"), None), P("sp", None)
    return jax.shard_map(step, mesh=mesh, in_specs=(tokens, P(None), whole, whole, whole, whole), out_specs=tokens, check_vma=False)
```

```python
import functools

import jax
import jax.numpy as jnp
from jax import lax
from jax.experimental import pallas as pl
from jax.experimental.pallas import tpu as pltpu
from jax.sharding import PartitionSpec as P


NEG = -1e30
HIDDEN = 2 * NEG
LOG2E = 1.4426950408889634
VMEM = 56 * 2**20
STRIP = 512
HEAD = 128
GROUP = 4
THETA = 10000
D = 2560
F32, BF16 = jnp.float32, jnp.bfloat16


def _dot(a, b, ca, cb):
    return lax.dot_general(a, b, (((ca,), (cb,)), ((), ())), preferred_element_type=F32)


def _attend(pos_ref, q_ref, k_ref, v_ref, *rest, causal, scale, bq, bk, carried):
    o_in, lse_in = rest[:2] if carried else (None, None)
    if carried:
        o_ref, top_s, mix_s = rest[-3:]
        lse_ref = gap_s = None
    else:
        o_ref, lse_ref, top_s, mix_s, gap_s = rest[-5:]
    kb, g, d = q_ref.shape[0], q_ref.shape[1], q_ref.shape[3]
    low = k_ref.dtype
    cols = g * bq
    iq = pl.program_id(0)
    e = scale * LOG2E
    wide = min(cols, STRIP)
    pieces = [(i, at) for i in range(kb) for at in range(0, cols, wide)]

    if causal:
        gap_s[...] = lax.rem(lax.broadcasted_iota(jnp.int32, (bk, cols), 1), bq) - lax.broadcasted_iota(jnp.int32, (bk, cols), 0)
    for i in range(kb):
        if carried:
            for n in range(g):
                h = i * g + n
                top_s[i : i + 1, n * bq : (n + 1) * bq] = jnp.maximum(lse_in[h : h + 1, :] * (1 / scale), NEG)
                mix_s[i, :d, n * bq : (n + 1) * bq] = o_in[:, h * d : (h + 1) * d].T
            mix_s[i, d:, :] = jnp.ones((8, cols), F32)
        else:
            top_s[i : i + 1, :] = jnp.full((1, cols), NEG, F32)
            mix_s[i] = jnp.zeros((d + 8, cols), F32)
    ones = jnp.ones((8, bk), low)

    def block(j, masked):
        here = pl.ds(j * bk, bk)
        scores = [_dot(k_ref[i, here, :], q_ref[i].reshape(cols, d)[at : at + wide, :], 1, 1) for i, at in pieces]
        ok = gap_s[...] >= j * bk - iq * bq if masked else None
        weights, keeps = [], []
        for (i, at), s in zip(pieces, scores):
            if masked:
                s = jnp.where(ok[:, at : at + wide], s, HIDDEN)
            old = top_s[i : i + 1, at : at + wide]
            top = jnp.maximum(old, s.max(axis=0, keepdims=True))
            top_s[i : i + 1, at : at + wide] = top
            weights.append(jnp.exp2((s - top) * e).astype(low))
            keeps.append(jnp.exp2((old - top) * e))
        for (i, at), p, keep in zip(pieces, weights, keeps):
            values = jnp.concatenate([v_ref[i, here, :].T, ones], axis=0)
            mix_s[i, :, at : at + wide] = mix_s[i, :, at : at + wide] * keep + _dot(values, p, 1, 0)

    if causal:
        whole, last = lax.div(iq * bq + 1, bk), lax.div(iq * bq + bq - 1 + bk, bk)
        lax.fori_loop(0, whole, lambda j, _: block(j, False), None)
        lax.fori_loop(whole, last, lambda j, _: block(j, True), None)
    else:
        lax.fori_loop(0, lax.div(pos_ref[0], bk), lambda j, _: block(j, False), None)

    for i in range(kb):
        top, total = top_s[i : i + 1, :], mix_s[i, d : d + 1, :]
        out = mix_s[i, :d, :] * (1 / total)
        if not carried:
            lse = top * scale + jnp.log(total)
        for n in range(g):
            h, part = i * g + n, slice(n * bq, (n + 1) * bq)
            o_ref[:, h * d : (h + 1) * d] = out[:, part].T.astype(o_ref.dtype)
            if not carried:
                lse_ref[h : h + 1, :] = lse[:, part]


def attend(q, kv, *, causal, keys=None, carry=None, bq=512, bk=512):
    kb, g, sq, d = q.shape
    sk = kv.shape[1]
    h = kb * g
    carried = carry is not None
    whole = lambda at: pl.BlockSpec((kb, sk, d), lambda iq, _: (at, 0, 0))
    rows = pl.BlockSpec((bq, h * d), lambda iq, _: (iq, 0))
    stats = pl.BlockSpec((h, bq), lambda iq, _: (0, iq))
    specs = [pl.BlockSpec((kb, g, bq, d), lambda iq, _: (0, 0, iq, 0)), whole(0), whole(1)] + ([rows, stats] if carried else [])
    out_shape = [jax.ShapeDtypeStruct((sq, h * d), BF16 if carried else F32)]
    out_specs = [rows]
    scratch = [pltpu.VMEM((kb, g * bq), F32), pltpu.VMEM((kb, d + 8, g * bq), F32)]
    if not carried:
        out_shape.append(jax.ShapeDtypeStruct((h, sq), F32))
        out_specs.append(stats)
        scratch.append(pltpu.VMEM((bk, g * bq), jnp.int32))
    keys = jnp.full((1,), sk if keys is None else keys, jnp.int32)
    out = pl.pallas_call(
        functools.partial(_attend, causal=causal, scale=d**-0.5, bq=bq, bk=bk, carried=carried),
        grid_spec=pltpu.PrefetchScalarGridSpec(num_scalar_prefetch=1, grid=(sq // bq,), in_specs=specs, out_specs=out_specs, scratch_shapes=scratch),
        out_shape=out_shape,
        compiler_params=pltpu.CompilerParams(dimension_semantics=("arbitrary",), vmem_limit_bytes=VMEM),
        cost_estimate=pl.CostEstimate(flops=4 * h * sq * sk * d // (2 if causal else 1), transcendentals=h * sq * sk, bytes_accessed=16 * 2**20),
        name="attend_far" if carried else "attend_near",
    )(keys, q, kv, kv, *(carry or ()))
    return out[0] if carried else out


def _place():
    g, sp = lax.axis_index("dp"), lax.axis_index("sp")
    return g, sp // 2, sp % 2


def _norm(core_ref, x_ref, gain_ref, *rest):
    wide = x_ref[...].astype(F32)
    scale = lax.rsqrt(jnp.mean(wide * wide, -1, keepdims=True) + 1e-6)
    rest[-1][...] = (wide * scale * gain_ref[...].astype(F32)).astype(BF16)


def norm(x, gain, c, into=None, bt=256):
    n = x.shape[0] // bt
    more = [] if into is None else [into]
    return pl.pallas_call(
        _norm,
        grid_spec=pltpu.PrefetchScalarGridSpec(
            num_scalar_prefetch=1, grid=(n,),
            in_specs=[pl.BlockSpec((bt, D), lambda j, core: (j, 0)), pl.BlockSpec((1, D), lambda j, core: (0, 0))] + [pl.BlockSpec(memory_space=pl.ANY)] * len(more),
            out_specs=pl.BlockSpec((bt, D), lambda j, core: (core[0] * n + j, 0))),
        out_shape=jax.ShapeDtypeStruct((2 * x.shape[0], D), BF16),
        input_output_aliases={3: 0} if more else {},
        compiler_params=pltpu.CompilerParams(dimension_semantics=("arbitrary",)),
        cost_estimate=pl.CostEstimate(flops=8 * x.size, transcendentals=0, bytes_accessed=4 * x.size),
        name="norm",
    )(jnp.full((1,), c, jnp.int32), x, gain.reshape(1, D), *more)


def _pack(wq_ref, wk_ref, wv_ref, *rest, wanted):
    outs, sems = rest[:-1], rest[-1]
    refs = (wq_ref, wk_ref, wv_ref)
    g, s, c = _place()
    n, waits = 0, []
    for out, want in zip(outs, wanted(g, s, c)):
        to = 0
        for ref, col, width in want:
            def copy(r, col=col, width=width, to=to, n=n, out=out):
                return pltpu.make_async_copy(r.at[:, pl.ds(pl.multiple_of(col, 128), width)], out.at[:, pl.ds(to, width)], sems.at[n])

            if ref < 3:
                copy(refs[ref]).start()
            else:
                @pl.when(g == 0)
                def _(copy=copy):
                    copy(wk_ref).start()

                @pl.when(g != 0)
                def _(copy=copy):
                    copy(wv_ref).start()
            waits.append(copy(refs[min(ref, 2)]))
            to += width
            n += 1
    for t in waits:
        t.wait()


def pack(wq, wk, wv, wanted):
    shapes = [(wq.shape[0], sum(w for _, _, w in want)) for want in wanted(0, 0, 0)]
    count = sum(len(want) for want in wanted(0, 0, 0))
    return pl.pallas_call(
        functools.partial(_pack, wanted=wanted),
        in_specs=[pl.BlockSpec(memory_space=pl.ANY)] * 3,
        out_shape=[jax.ShapeDtypeStruct(t, BF16) for t in shapes],
        out_specs=[pl.BlockSpec(memory_space=pltpu.VMEM)] * len(shapes),
        scratch_shapes=[pltpu.SemaphoreType.DMA((count,))],
        compiler_params=pltpu.CompilerParams(vmem_limit_bytes=16 * 2**20),
        cost_estimate=pl.CostEstimate(flops=2**20, transcendentals=0, bytes_accessed=4 * sum(a * b for a, b in shapes)),
    )(wq, wk, wv)


def _project(a_ref, cos_ref, sin_ref, *rest, plan):
    pieces, (q_ref, kv_ref, w_s, sems) = rest[:-4], rest[-4:]

    @pl.when(pl.program_id(0) == 0)
    def _():
        copies = []
        for n, (ref, col, width, row, to) in enumerate(plan):
            src = pieces[ref].at[:, pl.ds(col if isinstance(col, int) else pl.multiple_of(col, 128), width)]
            dst = w_s.at[pl.ds(pl.multiple_of(row, 128), src.shape[0]), pl.ds(to if isinstance(to, int) else pl.multiple_of(to, 128), width)]
            copies.append(pltpu.make_async_copy(src, dst, sems.at[n]))
        for copy in copies:
            copy.start()
        for copy in copies:
            copy.wait()

    cos, sin = cos_ref[...], sin_ref[...]
    acc = jnp.dot(a_ref[...], w_s[...], preferred_element_type=F32).astype(BF16)
    nq, nk = q_ref.shape[0], kv_ref.shape[0] // 2
    for h in range(nq + 2 * nk):
        t = acc[:, h * HEAD : (h + 1) * HEAD]
        if h < nq + nk:
            t = t.astype(F32)
            t = (t * cos + pltpu.roll(t, HEAD // 2, 1) * sin).astype(BF16)
        if h < nq:
            q_ref[h] = t
        else:
            kv_ref[h - nq] = t


def project(a, cos, sin, pieces, plan, kb, bt=256):
    tokens = a.shape[0]
    nq, nkv = kb * GROUP, 2 * kb
    width = (nq + nkv) * HEAD
    count = len(plan(0, 0, 0))
    return pl.pallas_call(
        lambda *refs: _project(*refs, plan=plan(*_place())),
        grid=(tokens // bt,),
        in_specs=[pl.BlockSpec((bt, D), lambda i: (i, 0))] + [pl.BlockSpec((bt, HEAD), lambda i: (i, 0))] * 2
        + [pl.BlockSpec(memory_space=pl.ANY)] * len(pieces),
        out_specs=[pl.BlockSpec((nq, bt, HEAD), lambda i: (0, i, 0)), pl.BlockSpec((nkv, bt, HEAD), lambda i: (0, i, 0))],
        out_shape=[jax.ShapeDtypeStruct((nq, tokens, HEAD), BF16), jax.ShapeDtypeStruct((nkv, tokens, HEAD), BF16)],
        scratch_shapes=[pltpu.VMEM((D, width), BF16), pltpu.SemaphoreType.DMA((count,))],
        compiler_params=pltpu.CompilerParams(dimension_semantics=("arbitrary",), vmem_limit_bytes=VMEM),
        cost_estimate=pl.CostEstimate(flops=2 * tokens * D * width, transcendentals=0, bytes_accessed=2 * (tokens * D + D * width + tokens * width)),
    )(a, cos, sin, *pieces)


def _finish(s0, s1, s2, own, wx0, wx1, wy0, wy1, x_ref, y_ref, w_s, seen_s, x_s, y_s, send_s, recv_s, load_sem, w_sem, send_sem, recv_sem, out_sem):
    g, s, c = _place()
    rows, width = 512, D // 2
    mate = {"sp": 2 * s + 1 - c}
    barrier = pltpu.get_barrier_semaphore()
    pl.semaphore_signal(barrier, inc=1, device_id=mate, device_id_type=pl.DeviceIdType.MESH)

    def seen_loads(which):
        first = pl.ds(pl.multiple_of((c if which else 1 - c) * 1024, 1024), 1024)
        at = 0
        for n, t in enumerate((s0, s1, s2)):
            yield pltpu.make_async_copy(t.at[first], seen_s.at[which, :, pl.ds(at, t.shape[1])], load_sem.at[3 * which + n])
            at += t.shape[1]

    def own_load(h):
        cols = pl.ds(h * width, width)
        return pltpu.make_async_copy(own.at[:, cols], w_s.at[pl.ds(pl.multiple_of(s * 1024, 1024), 1024), cols], w_sem.at[3 * h])

    def far_loads(h, parts):
        for n, t in enumerate(parts):
            there = w_s.at[pl.ds(pl.multiple_of((1 - s) * 1024 + n * 512, 512), 512), pl.ds(h * width, width)]
            yield pltpu.make_async_copy(t, there, w_sem.at[3 * h + 1 + n])

    def w_start(h):
        own_load(h).start()

        @pl.when(g == h)
        def _():
            for t in far_loads(h, (wx0, wx1)):
                t.start()

        @pl.when(g != h)
        def _():
            for t in far_loads(h, (wy0, wy1)):
                t.start()

    def w_wait(h):
        own_load(h).wait()
        for t in far_loads(h, (wx0, wx1)):
            t.wait()

    x_load = pltpu.make_async_copy(x_ref, x_s, load_sem.at[6])
    for t in seen_loads(0):
        t.start()
    w_start(0)
    w_start(1)
    for t in seen_loads(1):
        t.start()
    x_load.start()
    pl.semaphore_wait(barrier, 1)

    def spot(n):
        return pl.ds(pl.multiple_of(lax.rem(n, 2) * rows, rows), rows), pl.ds(pl.multiple_of(lax.div(n, 2) * width, 128), width)

    def part(which, n):
        at, cols = spot(n)
        return jnp.dot(seen_s[which, at, :], w_s[:, cols], preferred_element_type=F32)

    def parcel(n):
        return pltpu.make_async_remote_copy(src_ref=send_s.at[n], dst_ref=recv_s.at[n], send_sem=send_sem.at[n], recv_sem=recv_sem.at[n],
                                            device_id=mate, device_id_type=pl.DeviceIdType.MESH)

    def result(n):
        at, cols = spot(n)
        return pltpu.make_async_copy(y_s.at[at, cols], y_ref.at[at, cols], out_sem.at[n])

    for t in seen_loads(0):
        t.wait()
    w_wait(0)

    def for_mate(n, _):
        @pl.when(n == 2)
        def _():
            w_wait(1)

        send_s[n] = part(0, n)

        @pl.when(n > 0)
        def _():
            parcel(n - 1).start()

    lax.fori_loop(0, 4, for_mate, None)
    for t in seen_loads(1):
        t.wait()
    x_load.wait()
    parcel(3).start()

    def for_own(n, _):
        acc = part(1, n)
        parcel(n).wait()
        at, cols = spot(n)
        y_s[at, cols] = (x_s[at, cols].astype(F32) + (acc + recv_s[n])).astype(BF16)

        @pl.when(n > 0)
        def _():
            result(n - 1).start()

    lax.fori_loop(0, 4, for_own, None)
    result(3).start()
    for n in range(4):
        result(n).wait()


def finish(seen, wo, wx, wy, x):
    anywhere = pl.BlockSpec(memory_space=pl.ANY)
    args = [*seen, wo, *wx, *wy, x]
    return pl.pallas_call(
        _finish,
        in_specs=[anywhere] * len(args),
        out_specs=anywhere,
        out_shape=jax.ShapeDtypeStruct((1024, D), BF16),
        scratch_shapes=[pltpu.VMEM((2048, D), BF16), pltpu.VMEM((2, 1024, 2048), BF16), pltpu.VMEM((1024, D), BF16), pltpu.VMEM((1024, D), BF16),
                        pltpu.VMEM((4, 512, D // 2), F32), pltpu.VMEM((4, 512, D // 2), F32), pltpu.SemaphoreType.DMA((7,)), pltpu.SemaphoreType.DMA((6,)),
                        pltpu.SemaphoreType.DMA((4,)), pltpu.SemaphoreType.DMA((4,)), pltpu.SemaphoreType.DMA((4,))],
        compiler_params=pltpu.CompilerParams(collective_id=0, has_side_effects=True, vmem_limit_bytes=63 * 2**20),
        cost_estimate=pl.CostEstimate(flops=4 * 1024 * 2048 * D, transcendentals=0, bytes_accessed=30 * 2**20),
        name="finish",
    )(*args)


def _pairs(to):
    spots = [(g, s, c) for g in range(2) for s in range(2) for c in range(2)]
    flat = lambda t: 4 * t[0] + 2 * t[1] + t[2]
    return [(flat(t), flat(to(*t))) for t in spots if to(*t) is not None]


SAME = _pairs(lambda g, s, c: (g, 1 - s, c))
CROSS = _pairs(lambda g, s, c: (g, 1 - s, 1 - c))
MATE = _pairs(lambda g, s, c: (g, s, 1 - c))
TWIN = _pairs(lambda g, s, c: (1 - g, s, c))
AHEAD = _pairs(lambda g, s, c: (g, 1, c) if s == 0 else None)


def send(t, pairs):
    return lax.ppermute(t, ("dp", "sp"), pairs)


def step(x, gain, wq, wk, wv, wo):
    g, s, c = _place()
    own = x.shape[0]
    tokens = 2 * own
    units = ((0, (0,)), (0, (1,)), (1, (0, 1)))

    def share(unit, cc, half):
        a, rs = unit
        if len(rs) == 1:
            head = 4 * a + 2 * cc + rs[0]
            return [(0, head * 512 + half * 256, 256), (3, head * HEAD, HEAD)]
        head = 4 * a + 2 * cc + half
        return [(0, head * 512, 512), (1, head * HEAD, HEAD), (2, head * HEAD, HEAD)]

    def all_of(unit, cc):
        a, rs = unit
        n = len(rs)
        head = 4 * a + 2 * cc + rs[0]
        return [(0, head * 512, 512 * n), (1, head * HEAD, HEAD * n), (2, head * HEAD, HEAD * n)]

    def row(s, c):
        return (2 * s + c) * 640

    def plan_of(unit):
        n = len(unit[1])
        kv = 512 * n

        def plan(g, s, c):
            out, to = [], 0
            for ref, (_, col, width) in enumerate(all_of(unit, c)):
                out.append((ref, col, width, row(s, c), to))
                to += width
            out.append((3, 0, to, row(s, 1 - c), 0))
            for ref, (half, cc) in enumerate(((g, c), (g, 1 - c), (1 - g, c), (1 - g, 1 - c)), 4):
                if n == 1:
                    parts = [(0, 256, half * 256), (256, HEAD, kv + half * HEAD)]
                else:
                    parts = [(0, 512, half * 512), (512, HEAD, kv + half * HEAD), (512 + HEAD, HEAD, kv + (2 + half) * HEAD)]
                out += [(ref, col, width, row(1 - s, cc), to) for col, width, to in parts]
            return out

        return plan

    mate_x = send(x, MATE)
    far, mate = [], []
    for unit in units:
        got = pack(wq, wk, wv, lambda g, s, c, unit=unit: [share(unit, c, g), share(unit, 1 - c, g), all_of(unit, 1 - c)])
        far.append([send(t, pairs) for t, pairs in zip(got, (SAME, CROSS))])
        mate.append(send(got[2], MATE))

    def relay(n, m, after):
        piece, _ = lax.optimization_barrier((far[n][m], after))
        return send(piece, TWIN)

    half = norm(x, gain, c)
    first = relay(0, 0, half)
    act = norm(mate_x, gain, 1 - c, half)
    place = (s * tokens + jnp.arange(tokens)).astype(F32)
    angle = place[:, None] * THETA ** (-jnp.arange(HEAD // 2, dtype=F32) / (HEAD // 2))
    cos, sin = jnp.cos(angle), jnp.sin(angle)
    cos, sin = jnp.concatenate([cos, cos], 1), jnp.concatenate([-sin, sin], 1)

    def project_unit(n, twin, act):
        q, kv = project(act, cos, sin, [wq, wk, wv, mate[n], *far[n], *twin], plan_of(units[n]), len(units[n][1]))
        return q.reshape(-1, GROUP, tokens, HEAD), kv

    def near_unit(n):
        return attend(q[n], kv[n], causal=True)

    q, kv, near = [None] * 3, [None] * 3, [None] * 3
    twin = [[first, relay(0, 1, act)], [relay(1, 0, act)], []]
    q[0], kv[0] = project_unit(0, twin[0], act)
    twin[1].append(relay(1, 1, kv[0]))
    near[0] = near_unit(0)
    twin[2].append(relay(2, 0, near[0][1]))
    q[1], kv[1] = project_unit(1, twin[1], act)
    twin[2].append(relay(2, 1, kv[1]))
    near[1] = near_unit(1)
    q[2], kv[2] = project_unit(2, twin[2], lax.optimization_barrier((act, near[1][1]))[0])
    near[2] = near_unit(2)
    there = [send(t, AHEAD) for t in kv]

    wx, wy = [], []
    for n, after in enumerate((near[0][1], near[1][1])):
        part, _ = lax.optimization_barrier((wo, after))
        part = lax.dynamic_slice(part, (n * 512, g * (D // 2)), (512, D // 2))
        wx.append(send(part, SAME))
    seen = []
    for n in range(3):
        if n < 2:
            part, _ = lax.optimization_barrier((wx[n], near[2][1] if n == 0 else seen[0]))
            wy.append(send(part, TWIN))
        seen.append(attend(q[n], there[n], causal=False, keys=s * tokens, carry=near[n], bk=1024, bq=1024 if n < 2 else 512))

    return finish(seen, wo, wx, wy, x)


def solution(mesh):
    tokens, whole = P(("dp", "sp"), None), P("sp", None)
    return jax.shard_map(step, mesh=mesh, in_specs=(tokens, P(None), whole, whole, whole, whole), out_specs=tokens, check_vma=False)
```

```python
import functools

import jax
import jax.numpy as jnp
from jax import lax
from jax.experimental import pallas as pl
from jax.experimental.pallas import tpu as pltpu
from jax.sharding import PartitionSpec as P


NEG = -1e30
HIDDEN = 2 * NEG
LOG2E = 1.4426950408889634
VMEM = 56 * 2**20
STRIP = 512
HEAD = 128
GROUP = 4
THETA = 10000
D = 2560
F32, BF16 = jnp.float32, jnp.bfloat16


def _dot(a, b, ca, cb):
    return lax.dot_general(a, b, (((ca,), (cb,)), ((), ())), preferred_element_type=F32)


def _attend(on_ref, q_ref, *rest, scale, bq, near, far, carried, final):
    far_k, far_v, rest = (*rest[:2], rest[2:]) if far else (None, None, rest)
    near_k, near_v, rest = (*rest[:2], rest[2:]) if near else (None, None, rest)
    o_in, lse_in, rest = (*rest[:2], rest[2:]) if carried else (None, None, rest)
    o_ref, rest = rest[0], rest[1:]
    lse_ref, rest = (None, rest) if final else (rest[0], rest[1:])
    top_s, mix_s = rest[:2]
    g, d = q_ref.shape[1], q_ref.shape[3]
    cols = g * bq
    iq = pl.program_id(0)
    e = scale * LOG2E
    strips = range(0, cols, STRIP)

    if near:
        gap_s = rest[2]

        @pl.when(iq == 0)
        def _():
            gap_s[...] = lax.rem(lax.broadcasted_iota(jnp.int32, (near, cols), 1), bq) - lax.broadcasted_iota(jnp.int32, (near, cols), 0)
    if carried:
        for h in range(g):
            part = slice(h * bq, (h + 1) * bq)
            top_s[:, part] = jnp.maximum(lse_in[h : h + 1, :] * (1 / scale), NEG)
            mix_s[:d, part] = o_in[:, h * d : (h + 1) * d].T
        mix_s[d:, :] = jnp.ones((8, cols), F32)
    else:
        top_s[...] = jnp.full((1, cols), NEG, F32)
        mix_s[...] = jnp.zeros((d + 8, cols), F32)

    def block(k_ref, v_ref, j, bk, masked):
        here = pl.ds(j * bk, bk)
        scores = [_dot(k_ref[0, here, :], q_ref[0].reshape(cols, d)[at : at + STRIP, :], 1, 1) for at in strips]
        ok = gap_s[...] >= j * bk - iq * bq if masked else None
        weights, keeps = [], []
        for at, s in zip(strips, scores):
            if masked:
                s = jnp.where(ok[:, at : at + STRIP], s, HIDDEN)
            old = top_s[:, at : at + STRIP]
            top = jnp.maximum(old, s.max(axis=0, keepdims=True))
            top_s[:, at : at + STRIP] = top
            weights.append(jnp.exp2((s - top) * e).astype(BF16))
            keeps.append(jnp.exp2((old - top) * e))
        values = jnp.concatenate([v_ref[0, here, :].T, jnp.ones((8, bk), BF16)], axis=0)
        for at, p, keep in zip(strips, weights, keeps):
            mix_s[:, at : at + STRIP] = mix_s[:, at : at + STRIP] * keep + _dot(values, p, 1, 0)

    if far:
        lax.fori_loop(0, on_ref[0] * (far_k.shape[1] // far), lambda j, _: block(far_k, far_v, j, far, False), None)
    if near:
        whole, last = lax.div(iq * bq + 1, near), lax.div(iq * bq + bq - 1 + near, near)
        lax.fori_loop(0, on_ref[0] * whole, lambda j, _: block(near_k, near_v, j, near, False), None)
        lax.fori_loop(on_ref[0] * whole, on_ref[0] * last, lambda j, _: block(near_k, near_v, j, near, True), None)

    top, total = top_s[...], mix_s[d : d + 1, :]
    total = jnp.where(top > NEG, total, 1.0)
    out = mix_s[:d, :] * (1 / total)
    lse = None if final else top * scale + jnp.log(total)
    for h in range(g):
        part = slice(h * bq, (h + 1) * bq)
        o_ref[:, h * d : (h + 1) * d] = out[:, part].T.astype(o_ref.dtype)
        if not final:
            lse_ref[h : h + 1, :] = lse[:, part]


def attend(q, which, *, near=None, far=None, on=1, carry=None, final, bq, bk_near=512, bk_far=1024):
    _, g, sq, d = q.shape
    carried = carry is not None
    rows = pl.BlockSpec((bq, g * d), lambda iq, _: (iq, 0))
    stats = pl.BlockSpec((g, bq), lambda iq, _: (0, iq))
    specs, args, keys = [pl.BlockSpec((1, g, bq, d), lambda iq, _: (which, 0, iq, 0))], [q], 0
    for kv in (far, near):
        if kv is not None:
            specs += [pl.BlockSpec((1, kv.shape[1], d), lambda iq, _, at=at: (at, 0, 0)) for at in range(2)]
            args += [kv, kv]
            keys += kv.shape[1] // (1 if kv is far else 2)
    if carried:
        specs += [rows, stats]
        args += carry
    out_shape, out_specs = [jax.ShapeDtypeStruct((sq, g * d), BF16 if final else F32)], [rows]
    scratch = [pltpu.VMEM((1, g * bq), F32), pltpu.VMEM((d + 8, g * bq), F32)]
    if not final:
        out_shape.append(jax.ShapeDtypeStruct((g, sq), F32))
        out_specs.append(stats)
    if near is not None:
        scratch.append(pltpu.VMEM((bk_near, g * bq), jnp.int32))
    out = pl.pallas_call(
        functools.partial(_attend, scale=d**-0.5, bq=bq, near=bk_near if near is not None else 0, far=bk_far if far is not None else 0,
                          carried=carried, final=final),
        grid_spec=pltpu.PrefetchScalarGridSpec(num_scalar_prefetch=1, grid=(sq // bq,), in_specs=specs, out_specs=out_specs, scratch_shapes=scratch),
        out_shape=out_shape,
        compiler_params=pltpu.CompilerParams(dimension_semantics=("arbitrary",), vmem_limit_bytes=VMEM),
        cost_estimate=pl.CostEstimate(flops=4 * g * sq * keys * d, transcendentals=g * sq * keys, bytes_accessed=12 * 2**20),
        name="attend",
    )(jnp.full((1,), on, jnp.int32), *args)
    return out[0] if final else out


def _place():
    g, sp = lax.axis_index("dp"), lax.axis_index("sp")
    return g, sp // 2, sp % 2


def _norm(core_ref, x_ref, gain_ref, *rest):
    wide = x_ref[...].astype(F32)
    scale = lax.rsqrt(jnp.mean(wide * wide, -1, keepdims=True) + 1e-6)
    rest[-1][...] = (wide * scale * gain_ref[...].astype(F32)).astype(BF16)


def norm(x, gain, c, into=None, bt=256):
    n = x.shape[0] // bt
    more = [] if into is None else [into]
    return pl.pallas_call(
        _norm,
        grid_spec=pltpu.PrefetchScalarGridSpec(
            num_scalar_prefetch=1, grid=(n,),
            in_specs=[pl.BlockSpec((bt, D), lambda j, core: (j, 0)), pl.BlockSpec((1, D), lambda j, core: (0, 0))] + [pl.BlockSpec(memory_space=pl.ANY)] * len(more),
            out_specs=pl.BlockSpec((bt, D), lambda j, core: (core[0] * n + j, 0))),
        out_shape=jax.ShapeDtypeStruct((2 * x.shape[0], D), BF16),
        input_output_aliases={3: 0} if more else {},
        compiler_params=pltpu.CompilerParams(dimension_semantics=("arbitrary",)),
        cost_estimate=pl.CostEstimate(flops=8 * x.size, transcendentals=0, bytes_accessed=4 * x.size),
        name="norm",
    )(jnp.full((1,), c, jnp.int32), x, gain.reshape(1, D), *more)


def _pack(wq_ref, wk_ref, wv_ref, *rest, wanted):
    outs, sems = rest[:-1], rest[-1]
    refs = (wq_ref, wk_ref, wv_ref)
    g, s, c = _place()
    n, waits = 0, []
    for out, want in zip(outs, wanted(g, s, c)):
        to = 0
        for ref, col, width in want:
            def copy(r, col=col, width=width, to=to, n=n, out=out):
                return pltpu.make_async_copy(r.at[:, pl.ds(pl.multiple_of(col, 128), width)], out.at[:, pl.ds(to, width)], sems.at[n])

            if ref < 3:
                copy(refs[ref]).start()
            else:
                @pl.when(g == 0)
                def _(copy=copy):
                    copy(wk_ref).start()

                @pl.when(g != 0)
                def _(copy=copy):
                    copy(wv_ref).start()
            waits.append(copy(refs[min(ref, 2)]))
            to += width
            n += 1
    for t in waits:
        t.wait()


def pack(wq, wk, wv, wanted):
    shapes = [(wq.shape[0], sum(w for _, _, w in want)) for want in wanted(0, 0, 0)]
    count = sum(len(want) for want in wanted(0, 0, 0))
    return pl.pallas_call(
        functools.partial(_pack, wanted=wanted),
        in_specs=[pl.BlockSpec(memory_space=pl.ANY)] * 3,
        out_shape=[jax.ShapeDtypeStruct(t, BF16) for t in shapes],
        out_specs=[pl.BlockSpec(memory_space=pltpu.VMEM)] * len(shapes),
        scratch_shapes=[pltpu.SemaphoreType.DMA((count,))],
        compiler_params=pltpu.CompilerParams(vmem_limit_bytes=16 * 2**20),
        cost_estimate=pl.CostEstimate(flops=2**20, transcendentals=0, bytes_accessed=4 * sum(a * b for a, b in shapes)),
    )(wq, wk, wv)


def _project(a_ref, cos_ref, sin_ref, *rest, plan, groups):
    pieces, (q_ref, *kv_refs, w_s, sems) = rest[:-3 - groups], rest[-3 - groups:]

    @pl.when(pl.program_id(0) == 0)
    def _():
        copies = []
        for n, (ref, col, width, row, to) in enumerate(plan):
            src = pieces[ref].at[:, pl.ds(col if isinstance(col, int) else pl.multiple_of(col, 128), width)]
            dst = w_s.at[pl.ds(pl.multiple_of(row, 128), src.shape[0]), pl.ds(to if isinstance(to, int) else pl.multiple_of(to, 128), width)]
            copies.append(pltpu.make_async_copy(src, dst, sems.at[n]))
        for copy in copies:
            copy.start()
        for copy in copies:
            copy.wait()

    cos, sin = cos_ref[...], sin_ref[...]
    acc = jnp.dot(a_ref[...], w_s[...], preferred_element_type=F32).astype(BF16)
    nq, nk = q_ref.shape[0], groups
    for h in range(nq + 2 * nk):
        t = acc[:, h * HEAD : (h + 1) * HEAD]
        if h < nq + nk:
            t = t.astype(F32)
            t = (t * cos + pltpu.roll(t, HEAD // 2, 1) * sin).astype(BF16)
        if h < nq:
            q_ref[h] = t
        else:
            kv_refs[(h - nq) % nk][(h - nq) // nk] = t


def project(a, cos, sin, pieces, plan, kb, bt=256):
    tokens = a.shape[0]
    nq = kb * GROUP
    width = (nq + 2 * kb) * HEAD
    count = len(plan(0, 0, 0))
    return pl.pallas_call(
        lambda *refs: _project(*refs, plan=plan(*_place()), groups=kb),
        grid=(tokens // bt,),
        in_specs=[pl.BlockSpec((bt, D), lambda i: (i, 0))] + [pl.BlockSpec((bt, HEAD), lambda i: (i, 0))] * 2
        + [pl.BlockSpec(memory_space=pl.ANY)] * len(pieces),
        out_specs=[pl.BlockSpec((nq, bt, HEAD), lambda i: (0, i, 0))] + [pl.BlockSpec((2, bt, HEAD), lambda i: (0, i, 0))] * kb,
        out_shape=[jax.ShapeDtypeStruct((nq, tokens, HEAD), BF16)] + [jax.ShapeDtypeStruct((2, tokens, HEAD), BF16)] * kb,
        scratch_shapes=[pltpu.VMEM((D, width), BF16), pltpu.SemaphoreType.DMA((count,))],
        compiler_params=pltpu.CompilerParams(dimension_semantics=("arbitrary",), vmem_limit_bytes=VMEM),
        cost_estimate=pl.CostEstimate(flops=2 * tokens * D * width, transcendentals=0, bytes_accessed=2 * (tokens * D + D * width + tokens * width)),
    )(a, cos, sin, *pieces)


def _finish(s0, t0, s1, s2, s3, own, wx0, wx1, wy0, wy1, x_ref, y_ref, w_s, seen_s, x_s, y_s, send_s, recv_s, load_sem, w_sem, send_sem, recv_sem, out_sem):
    g, s, c = _place()
    rows, width = 512, D // 2
    mate = {"sp": 2 * s + 1 - c}
    barrier = pltpu.get_barrier_semaphore()
    pl.semaphore_signal(barrier, inc=1, device_id=mate, device_id_type=pl.DeviceIdType.MESH)

    def seen_load(which, n, t):
        first = pl.ds(pl.multiple_of((c if which else 1 - c) * 1024, 1024), 1024)
        return pltpu.make_async_copy(t.at[first], seen_s.at[which, :, pl.ds(n * 512, 512)], load_sem.at[4 * which + n])

    def seen_start(which):
        @pl.when(s == 0)
        def _():
            seen_load(which, 0, s0).start()

        @pl.when(s != 0)
        def _():
            seen_load(which, 0, t0).start()

        for n, t in enumerate((s1, s2, s3), 1):
            seen_load(which, n, t).start()

    def seen_wait(which):
        for n, t in enumerate((s0, s1, s2, s3)):
            seen_load(which, n, t).wait()

    def own_load(h):
        cols = pl.ds(h * width, width)
        return pltpu.make_async_copy(own.at[:, cols], w_s.at[pl.ds(pl.multiple_of(s * 1024, 1024), 1024), cols], w_sem.at[3 * h])

    def far_loads(h, parts):
        for n, t in enumerate(parts):
            there = w_s.at[pl.ds(pl.multiple_of((1 - s) * 1024 + n * 512, 512), 512), pl.ds(h * width, width)]
            yield pltpu.make_async_copy(t, there, w_sem.at[3 * h + 1 + n])

    def w_start(h):
        own_load(h).start()

        @pl.when(g == h)
        def _():
            for t in far_loads(h, (wx0, wx1)):
                t.start()

        @pl.when(g != h)
        def _():
            for t in far_loads(h, (wy0, wy1)):
                t.start()

    def w_wait(h):
        own_load(h).wait()
        for t in far_loads(h, (wx0, wx1)):
            t.wait()

    x_load = pltpu.make_async_copy(x_ref, x_s, load_sem.at[8])
    seen_start(0)
    w_start(0)
    w_start(1)
    seen_start(1)
    x_load.start()
    pl.semaphore_wait(barrier, 1)

    def spot(n):
        return pl.ds(pl.multiple_of(lax.rem(n, 2) * rows, rows), rows), pl.ds(pl.multiple_of(lax.div(n, 2) * width, 128), width)

    def part(which, n):
        at, cols = spot(n)
        return jnp.dot(seen_s[which, at, :], w_s[:, cols], preferred_element_type=F32)

    def parcel(n):
        return pltpu.make_async_remote_copy(src_ref=send_s.at[n], dst_ref=recv_s.at[n], send_sem=send_sem.at[n], recv_sem=recv_sem.at[n],
                                            device_id=mate, device_id_type=pl.DeviceIdType.MESH)

    def result(n):
        at, cols = spot(n)
        return pltpu.make_async_copy(y_s.at[at, cols], y_ref.at[at, cols], out_sem.at[n])

    seen_wait(0)
    w_wait(0)

    def for_mate(n, _):
        @pl.when(n == 2)
        def _():
            w_wait(1)

        send_s[n] = part(0, n)

        @pl.when(n > 0)
        def _():
            parcel(n - 1).start()

    lax.fori_loop(0, 4, for_mate, None)
    seen_wait(1)
    x_load.wait()
    parcel(3).start()

    def for_own(n, _):
        acc = part(1, n)
        parcel(n).wait()
        at, cols = spot(n)
        y_s[at, cols] = (x_s[at, cols].astype(F32) + (acc + recv_s[n])).astype(BF16)

        @pl.when(n > 0)
        def _():
            result(n - 1).start()

    lax.fori_loop(0, 4, for_own, None)
    result(3).start()
    for n in range(4):
        result(n).wait()


def finish(seen, wo, wx, wy, x):
    anywhere = pl.BlockSpec(memory_space=pl.ANY)
    args = [*seen, wo, *wx, *wy, x]
    return pl.pallas_call(
        _finish,
        in_specs=[anywhere] * len(args),
        out_specs=anywhere,
        out_shape=jax.ShapeDtypeStruct((1024, D), BF16),
        scratch_shapes=[pltpu.VMEM((2048, D), BF16), pltpu.VMEM((2, 1024, 2048), BF16), pltpu.VMEM((1024, D), BF16), pltpu.VMEM((1024, D), BF16),
                        pltpu.VMEM((4, 512, D // 2), F32), pltpu.VMEM((4, 512, D // 2), F32), pltpu.SemaphoreType.DMA((9,)), pltpu.SemaphoreType.DMA((6,)),
                        pltpu.SemaphoreType.DMA((4,)), pltpu.SemaphoreType.DMA((4,)), pltpu.SemaphoreType.DMA((4,))],
        compiler_params=pltpu.CompilerParams(collective_id=0, has_side_effects=True, vmem_limit_bytes=63 * 2**20),
        cost_estimate=pl.CostEstimate(flops=4 * 1024 * 2048 * D, transcendentals=0, bytes_accessed=30 * 2**20),
        name="finish",
    )(*args)


def _pairs(to):
    spots = [(g, s, c) for g in range(2) for s in range(2) for c in range(2)]
    flat = lambda t: 4 * t[0] + 2 * t[1] + t[2]
    return [(flat(t), flat(to(*t))) for t in spots if to(*t) is not None]


SAME = _pairs(lambda g, s, c: (g, 1 - s, c))
CROSS = _pairs(lambda g, s, c: (g, 1 - s, 1 - c))
MATE = _pairs(lambda g, s, c: (g, s, 1 - c))
TWIN = _pairs(lambda g, s, c: (1 - g, s, c))
BACK = _pairs(lambda g, s, c: (g, 0, c) if s == 1 else None)
AHEAD = _pairs(lambda g, s, c: (g, 1, c) if s == 0 else None)


def send(t, pairs):
    return lax.ppermute(t, ("dp", "sp"), pairs)


def step(x, gain, wq, wk, wv, wo):
    g, s, c = _place()
    own = x.shape[0]
    tokens = 2 * own
    units = ((0, (0,)), (0, (1,)), (1, (0, 1)))

    def share(unit, cc, half):
        a, rs = unit
        if len(rs) == 1:
            head = 4 * a + 2 * cc + rs[0]
            return [(0, head * 512 + half * 256, 256), (3, head * HEAD, HEAD)]
        head = 4 * a + 2 * cc + half
        return [(0, head * 512, 512), (1, head * HEAD, HEAD), (2, head * HEAD, HEAD)]

    def all_of(unit, cc):
        a, rs = unit
        n = len(rs)
        head = 4 * a + 2 * cc + rs[0]
        return [(0, head * 512, 512 * n), (1, head * HEAD, HEAD * n), (2, head * HEAD, HEAD * n)]

    def row(s, c):
        return (2 * s + c) * 640

    def plan_of(unit):
        n = len(unit[1])
        kv = 512 * n

        def plan(g, s, c):
            out, to = [], 0
            for ref, (_, col, width) in enumerate(all_of(unit, c)):
                out.append((ref, col, width, row(s, c), to))
                to += width
            out.append((3, 0, to, row(s, 1 - c), 0))
            for ref, (half, cc) in enumerate(((g, c), (g, 1 - c), (1 - g, c), (1 - g, 1 - c)), 4):
                if n == 1:
                    parts = [(0, 256, half * 256), (256, HEAD, kv + half * HEAD)]
                else:
                    parts = [(0, 512, half * 512), (512, HEAD, kv + half * HEAD), (512 + HEAD, HEAD, kv + (2 + half) * HEAD)]
                out += [(ref, col, width, row(1 - s, cc), to) for col, width, to in parts]
            return out

        return plan

    mate_x = send(x, MATE)
    far, mate = [], []
    for unit in units:
        got = pack(wq, wk, wv, lambda g, s, c, unit=unit: [share(unit, c, g), share(unit, 1 - c, g), all_of(unit, 1 - c)])
        far.append([send(t, pairs) for t, pairs in zip(got, (SAME, CROSS))])
        mate.append(send(got[2], MATE))

    def relay(n, m, after):
        piece, _ = lax.optimization_barrier((far[n][m], after))
        return send(piece, TWIN)

    half = norm(x, gain, c)
    first = relay(0, 0, half)
    act = norm(mate_x, gain, 1 - c, half)
    place = (s * tokens + jnp.arange(tokens)).astype(F32)
    angle = place[:, None] * THETA ** (-jnp.arange(HEAD // 2, dtype=F32) / (HEAD // 2))
    cos, sin = jnp.cos(angle), jnp.sin(angle)
    cos, sin = jnp.concatenate([cos, cos], 1), jnp.concatenate([-sin, sin], 1)

    def project_unit(n, twin, act):
        q, *kv = project(act, cos, sin, [wq, wk, wv, mate[n], *far[n], *twin], plan_of(units[n]), len(units[n][1]))
        return q.reshape(-1, GROUP, tokens, HEAD), kv

    half = norm(x, gain, c)
    first = relay(0, 0, half)
    act = norm(mate_x, gain, 1 - c, half)
    place = (s * tokens + jnp.arange(tokens)).astype(F32)
    angle = place[:, None] * THETA ** (-jnp.arange(HEAD // 2, dtype=F32) / (HEAD // 2))
    cos, sin = jnp.cos(angle), jnp.sin(angle)
    cos, sin = jnp.concatenate([cos, cos], 1), jnp.concatenate([-sin, sin], 1)

    def tied(value, after):
        return lax.optimization_barrier((value, after))[0]

    def near_group(n, q, which):
        return attend(q, which, near=kv[n], final=False, bq=512)

    first_chip = 1 - s
    twin = [[first, relay(0, 1, act)], [relay(1, 0, act)], []]
    kv, near = [None] * 4, [None] * 4
    q0, (kv[0],) = project_unit(0, twin[0], act)
    lent = send(q0, BACK), send(kv[0], BACK)
    twin[1].append(relay(1, 1, kv[0]))
    own0 = attend(q0, 0, near=kv[0], on=first_chip, final=True, bq=512)
    twin[2].append(relay(2, 0, own0))
    q1, (kv[1],) = project_unit(1, twin[1], tied(act, own0))
    twin[2].append(relay(2, 1, kv[1]))
    near[1] = near_group(1, q1, 0)
    q2, kv[2:] = project_unit(2, twin[2], tied(act, near[1][1]))
    near[2] = near_group(2, q2, 0)
    back0 = attend(tied(lent[0], near[2][1]), 0, near=lent[1], far=kv[0], on=first_chip, final=True, bq=512, bk_far=512)
    near[3] = near_group(3, tied(q2, back0), 1)
    there = [None] + [send(kv[n], AHEAD) for n in range(1, 4)]

    wx, wy = [], []
    for n, after in enumerate((kv[1], kv[3])):
        part = lax.dynamic_slice(tied(wo, after), (n * 512, g * (D // 2)), (512, D // 2))
        wx.append(send(part, SAME))
    seen0 = send(back0, AHEAD)
    wy.append(send(tied(wx[0], near[3][1]), TWIN))
    seen = [own0, seen0]
    for n in range(1, 4):
        if n == 3:
            wy.append(send(tied(wx[1], seen[-1]), TWIN))
        q, which = ((q1, 0), (q2, 0), (q2, 1))[n - 1]
        q = q if n == 1 else tied(q, seen[-1])
        seen.append(attend(q, which, far=there[n], on=s, carry=near[n], final=True, bq=1024))
    return finish(seen, wo, wx, wy, x)


def solution(mesh):
    tokens, whole = P(("dp", "sp"), None), P("sp", None)
    return jax.shard_map(step, mesh=mesh, in_specs=(tokens, P(None), whole, whole, whole, whole), out_specs=tokens, check_vma=False)
```
